32 devices in a mesh: fsdp: 8 (over y, x, core), seq: 4 (over z).
Axes of the slice: x: 2, y: 2, z: 4, core: 2. Of those that a mesh axis runs over, the one named last changes fastest.
Arguments:
- tokens: bfloat16 [8, 2048, 4096], P('fsdp', 'seq'), may hold values from -72 to 72
- norm_gain: float32 [4096], replicated, may hold values from 0.1 to 1.9
- lru_proj: bfloat16 [4096, 2048], P(('fsdp', 'seq')), may hold values from -0.09375 to 0.09375
- gelu_proj: bfloat16 [4096, 2048], P(('fsdp', 'seq')), may hold values from -0.09375 to 0.09375
- conv_weight: float32 [4, 2048], replicated, may hold values from -3 to 3
- conv_bias: float32 [2048], replicated, may hold values from -3 to 3
- gate_weights: bfloat16 [2048, 512], P('seq'), may hold values from -0.375 to 0.375
- gate_bias: float32 [2, 2048], replicated, may hold values from -4 to 4
- decay_param: float32 [2048], replicated, may hold values from -13 to -2
Outputs:
- recurrent_out: bfloat16 [8, 2048, 2048], P('fsdp', 'seq')
The draws below stay inside these ranges and needn't reach their ends.
All inputs are finite; a program needn't handle non-finite values.
Results may differ from the reference program's by a relative error of at most 0.0051.
Values may be sent and summed in bfloat16 or wider, within the bound.
No kernel may reach another device: no remote copies, remote signals or barrier semaphores. Data moves between devices by JAX's collectives and lax.ppermute only.
A program may use at most 128 MiB of HBM per device.

```python
import math
import jax
import jax.numpy as jnp
from jax import lax

D = 4096
BW = 256
H = 8
CONV = 4
TOK_DEV = 512
C = 2048
LENGTH = 2048
SEQS = 8


def draw_tokens(key, part):
    keys = jax.random.split(key, 3)
    shape = (SEQS, LENGTH, D)
    column_scale = jnp.exp(jax.random.uniform(keys[0], (D,), jnp.float32, math.log(0.3), math.log(3.0)))
    row_scale = jnp.exp(jax.random.uniform(keys[1], (SEQS, LENGTH, 1), jnp.float32, math.log(0.3), math.log(3.0)))
    base = jnp.clip(jax.random.normal(keys[2], shape, jnp.float32), -3.0, 3.0)
    return (base * row_scale * column_scale).astype(jnp.bfloat16)


def draw_decay_param(key, part):
    keys = jax.random.split(key, 3)
    shortest = min(40, TOK_DEV)
    slow_rate = jnp.exp(jax.random.uniform(keys[0], (C,), jnp.float32, math.log(0.05 / LENGTH), math.log(0.5 / LENGTH)))
    fast_rate = jnp.exp(jax.random.uniform(keys[1], (C,), jnp.float32, math.log(0.2 / shortest), math.log(0.5 / shortest)))
    share = 0.5
    picked = jax.random.uniform(keys[2], (C,), jnp.float32) < share
    rate = jnp.where(picked, fast_rate, slow_rate)
    return jnp.log(jnp.expm1(rate)).astype(jnp.float32)


def block_levels(key, dims, cuts, smallest, high):
    def one(position, blocks):
        draws = jax.random.uniform(jax.random.fold_in(jax.random.fold_in(key, 6), position), (blocks,), jnp.float32, smallest / len(cuts), high / len(cuts))
        return jnp.repeat(jnp.exp(draws), dims[position] // blocks).reshape((-1,) + (1,) * (len(dims) - position - 1))

    factor_of = one(*cuts[0])
    for cut in cuts[1:]:
        factor_of = factor_of * one(*cut)
    return factor_of


def noise(stream_key, extent, width, bound, cuts=(), kind=jnp.bfloat16):
    values = jax.random.normal(stream_key, extent, jnp.float32) * width
    if len(cuts) > 0:
        values = block_levels(stream_key, extent, cuts, -0.22, 0.18) * values
    return jnp.clip(values, min=-bound, max=bound).astype(kind)


def setup_inputs(seed: int = 0) -> dict:
    streams_of = jax.random.split(jax.random.key(seed), 10)
    return {
        "tokens": draw_tokens(jax.random.fold_in(streams_of[9], 71), 0),
        "norm_gain": jnp.clip(1.0 + 0.18 * jax.random.normal(streams_of[1], (D,), jnp.float32), 0.1, 1.9),
        "lru_proj": noise(streams_of[2], (D, C), D ** -0.5, 0.09375, ((0, 32),)),
        "gelu_proj": noise(streams_of[3], (D, C), D ** -0.5, 0.09375, ((0, 32),)),
        "conv_weight": noise(streams_of[4], (CONV, C), 0.5, 3.0, (), jnp.float32),
        "conv_bias": noise(streams_of[5], (C,), 0.5, 3.0, (), jnp.float32),
        "gate_weights": noise(streams_of[6], (C, 2 * BW), BW ** -0.5, 0.375, ((0, 4),)),
        "gate_bias": noise(streams_of[7], (2, C), 1.0, 4.0, (), jnp.float32),
        "decay_param": draw_decay_param(jax.random.fold_in(streams_of[9], 71), 0),
    }


def reference(tokens, norm_gain, lru_proj, gelu_proj, conv_weight, conv_bias, gate_weights, gate_bias, decay_param):

    def one_sequence(rows):
        values = rows.astype(jnp.float32)
        mean_square = lax.optimization_barrier(jnp.mean(values * values, axis=-1, keepdims=True))
        normed = (values * lax.rsqrt(mean_square + 1e-06) * norm_gain).astype(jnp.bfloat16)
        recurrent_in = jnp.dot(normed, lru_proj, preferred_element_type=jnp.float32).astype(jnp.bfloat16)
        gelu_in = jnp.dot(normed, gelu_proj, preferred_element_type=jnp.float32)
        padded = jnp.concatenate([jnp.zeros((CONV - 1, C), jnp.bfloat16), recurrent_in], axis=0)
        conv_sum = jnp.zeros((LENGTH, C), jnp.float32) + conv_bias
        for tap_index in range(CONV):
            begin = CONV - 1 - tap_index
            conv_sum = conv_sum + conv_weight[tap_index] * padded[begin:begin + LENGTH].astype(jnp.float32)
        conv_out = conv_sum.astype(jnp.bfloat16)
        gate_all = jnp.einsum('lhi,hij->lhj', conv_out.astype(jnp.float32).reshape(LENGTH, H, BW), gate_weights.astype(jnp.float32).reshape(H, BW, 2 * BW))
        input_gate = jax.nn.sigmoid(gate_all[:, :, :BW].reshape(LENGTH, C) + gate_bias[0])
        recur_gate = jax.nn.sigmoid(gate_all[:, :, BW:].reshape(LENGTH, C) + gate_bias[1])
        log_decay = -8.0 * jax.nn.softplus(decay_param) * recur_gate
        decay = jnp.exp(log_decay)
        driven = jnp.sqrt(-jnp.expm1(2.0 * log_decay)) * input_gate * conv_out.astype(jnp.float32)

        def advance(state, inputs):
            decay_now, driven_now = inputs
            state = decay_now * state + driven_now
            return (state, state)
        unused, states = lax.scan(advance, jnp.zeros((C,), jnp.float32), (decay, driven))
        return (states * jax.nn.gelu(gelu_in, approximate=True)).astype(jnp.bfloat16)
    return lax.map(one_sequence, tokens)
```

```python
import functools

import jax
import jax.numpy as jnp
from jax import lax
from jax.experimental import pallas as pl
from jax.experimental.pallas import tpu as pltpu
from jax.sharding import PartitionSpec as P

LRU_CHUNKS = 2
GELU_CHUNKS = 2
BF = jnp.bfloat16
F32 = jnp.float32


def params(*kinds):
    return pltpu.CompilerParams(dimension_semantics=kinds, vmem_limit_bytes=56 * 1024 * 1024)


def flip(x, bit):
    return lax.ppermute(x, "fsdp", [(i, i ^ bit) for i in range(lax.axis_size("fsdp"))])


def line_gather(x):
    devices = lax.axis_size("seq")
    right, left = x, x
    below, above = [], []
    for hop in range(1, devices):
        right = lax.ppermute(right, "seq", [(i, i + 1) for i in range(hop - 1, devices - 1)])
        left = lax.ppermute(left, "seq", [(i, i - 1) for i in range(1, devices - hop + 1)])
        below.append(right)
        above.append(left)
    stacked = jnp.stack(below[::-1] + [x] + above)
    begin = devices - 1 - lax.axis_index("seq")
    return lax.dynamic_slice_in_dim(stacked, begin, devices, axis=0)


def plane_gather(block, bits):
    found = {0: block}
    for bit in bits:
        found.update({offset ^ bit: flip(part, bit) for offset, part in list(found.items())})
    return found


def norm_body(order, own, other, gain, out, scratch):
    block = out.shape[2] // order.shape[0]
    for source, index in ((own, 0), (other, 1)):
        values = source[...].astype(F32)
        mean_square = jnp.mean(values * values, axis=-1, keepdims=True)
        scratch[...] = (values * lax.rsqrt(mean_square + 1e-06) * gain[...]).astype(BF)
        for position in range(order.shape[0]):
            begin = pl.multiple_of(order[position] * block, 128)
            out[index, :, position * block : (position + 1) * block] = scratch[:, pl.ds(begin, block)]


def norm(own, other, gain, order):
    rows, width = own.shape
    step = 128
    return pl.pallas_call(
        norm_body,
        grid_spec=pltpu.PrefetchScalarGridSpec(
            num_scalar_prefetch=1,
            grid=(rows // step,),
            in_specs=[
                pl.BlockSpec((step, width), lambda i, o: (i, 0)),
                pl.BlockSpec((step, width), lambda i, o: (i, 0)),
                pl.BlockSpec((1, width), lambda i, o: (0, 0)),
            ],
            out_specs=pl.BlockSpec((2, step, width), lambda i, o: (0, i, 0)),
            scratch_shapes=[pltpu.VMEM((step, width), BF)],
        ),
        out_shape=jax.ShapeDtypeStruct((2, rows, width), BF),
        compiler_params=params("arbitrary"),
        name="norm",
    )(order, own, other, gain.reshape(1, -1)).reshape(2 * rows, width)


def load_table(parts, table, sems):
    @pl.when(pl.program_id(0) == 0)
    def _():
        height = parts[0].shape[0]
        copies = [
            pltpu.make_async_copy(part, table.at[pl.ds(i * height, height)], sems.at[i])
            for i, part in enumerate(parts)
        ]
        for copy in copies:
            copy.start()
        for copy in copies:
            copy.wait()


def product_body(count, rows, *refs):
    parts, out, table, sems = refs[:count], refs[count], refs[count + 1], refs[count + 2]
    load_table(parts, table, sems)
    out[...] = jnp.dot(rows[...], table[...], preferred_element_type=F32).astype(out.dtype)


def gelu_tanh(v):
    return 0.5 * v * (1.0 + jnp.tanh(0.7978845608028654 * (v + 0.044715 * v * v * v)))


def finish_body(count, rows, local, cumulative, start, *refs):
    parts, out, table, sems = refs[:count], refs[count], refs[count + 1], refs[count + 2]
    load_table(parts, table, sems)
    gelu_in = jnp.dot(rows[...], table[...], preferred_element_type=F32)
    state = local[...] + cumulative[...] * start[0]
    out[...] = (state * gelu_tanh(gelu_in)).astype(BF)


def product(rows, parts):
    total, depth = rows.shape
    width = parts[0].shape[1]
    step = 256
    count = len(parts)
    return pl.pallas_call(
        functools.partial(product_body, count),
        grid=(total // step,),
        in_specs=[pl.BlockSpec((step, depth), lambda i: (i, 0))]
        + [pl.BlockSpec(memory_space=pl.ANY)] * count,
        out_specs=pl.BlockSpec((step, width), lambda i: (i, 0)),
        out_shape=jax.ShapeDtypeStruct((total, width), BF),
        scratch_shapes=[pltpu.VMEM((depth, width), BF), pltpu.SemaphoreType.DMA((count,))],
        compiler_params=params("arbitrary"),
        name="lru_product",
    )(rows, *parts)


def finish(rows, parts, local, cumulative, start, column, first, some):
    depth = rows.shape[1]
    width = parts[0].shape[1]
    step = 256
    count = len(parts)
    base = first // step
    per_start = local.shape[0] // start.shape[0] // step
    return pl.pallas_call(
        functools.partial(finish_body, count),
        grid=(some // step,),
        in_specs=[
            pl.BlockSpec((step, depth), lambda i: (i + base, 0)),
            pl.BlockSpec((step, width), lambda i: (i + base, column)),
            pl.BlockSpec((step, width), lambda i: (i + base, column)),
            pl.BlockSpec((1, 1, width), lambda i: ((i + base) // per_start, 0, column)),
        ]
        + [pl.BlockSpec(memory_space=pl.ANY)] * count,
        out_specs=pl.BlockSpec((step, width), lambda i: (i, 0)),
        out_shape=jax.ShapeDtypeStruct((some, width), BF),
        scratch_shapes=[pltpu.VMEM((depth, width), BF), pltpu.SemaphoreType.DMA((count,))],
        compiler_params=params("arbitrary"),
        name="gelu_finish",
    )(rows, local, cumulative, start, *parts)


def minus_expm1(y):
    series = -y * (1.0 + y * (0.5 + y * (1 / 6 + y * (1 / 24 + y * (1 / 120)))))
    return jnp.where(y > -0.1, series, 1.0 - jnp.exp(y))


def recur_body(before, rin, taps, bias, table, gate_bias, slope, local, cumulative, padded, decay, driven, carry):
    step, inner = rin.shape
    heads, block = table.shape[0], table.shape[1]

    @pl.when(pl.program_id(1) == 0)
    def _():
        padded[0:8, :] = before[0].astype(F32)
        carry[0:8, :] = jnp.zeros((8, inner), F32)
        carry[8:16, :] = jnp.ones((8, inner), F32)

    padded[8 : 8 + step, :] = rin[...].astype(F32)
    for head in range(heads):
        at = slice(head * block, (head + 1) * block)
        conv_sum = jnp.broadcast_to(bias[0:1, at], (step, block))
        for tap in range(taps.shape[0]):
            conv_sum = conv_sum + taps[tap : tap + 1, at] * padded[8 - tap : 8 - tap + step, at]
        conv_out = conv_sum.astype(BF)
        gates = jnp.dot(conv_out, table[head], preferred_element_type=F32)
        input_gate = jax.nn.sigmoid(gates[:, :block] + gate_bias[0:1, at])
        recur_gate = jax.nn.sigmoid(gates[:, block:] + gate_bias[1:2, at])
        log_decay = slope[0:1, at] * recur_gate
        decay[:, at] = jnp.exp(log_decay)
        driven[:, at] = jnp.sqrt(minus_expm1(2.0 * log_decay)) * input_gate * conv_out.astype(F32)
    padded[0:8, :] = padded[step : step + 8, :]
    row = lax.broadcasted_iota(jnp.int32, (8, inner), 0)

    def advance(group, carried):
        state, prefix = carried
        at = pl.ds(pl.multiple_of(group * 8, 8), 8)
        a, b = decay[at, :], driven[at, :]
        for shift in (1, 2, 4):
            keep = row >= shift
            b = b + a * jnp.where(keep, pltpu.roll(b, shift, 0), 0.0)
            a = a * jnp.where(keep, pltpu.roll(a, shift, 0), 1.0)
        state = b + a * state
        prefix = a * prefix
        local[at, :] = state
        cumulative[at, :] = prefix
        return (
            jnp.broadcast_to(state[7:8, :], (8, inner)),
            jnp.broadcast_to(prefix[7:8, :], (8, inner)),
        )

    state, prefix = lax.fori_loop(0, step // 8, advance, (carry[0:8, :], carry[8:16, :]))
    carry[0:8, :] = state
    carry[8:16, :] = prefix


def recur(rin, before, taps, bias, table, gate_bias, slope):
    total, inner = rin.shape
    seqs = before.shape[0]
    step = 128
    blocks = total // seqs // step
    whole = lambda shape: pl.BlockSpec(shape, lambda s, t: (0,) * len(shape))
    rows = pl.BlockSpec((step, inner), lambda s, t: (s * blocks + t, 0))
    return pl.pallas_call(
        recur_body,
        grid=(seqs, blocks),
        in_specs=[
            pl.BlockSpec((1, 8, inner), lambda s, t: (s, 0, 0)),
            rows,
            whole(taps.shape),
            whole((1, inner)),
            whole(table.shape),
            whole((2, inner)),
            whole((1, inner)),
        ],
        out_specs=[rows, rows],
        out_shape=[jax.ShapeDtypeStruct((total, inner), F32)] * 2,
        scratch_shapes=[
            pltpu.VMEM((step + 8, inner), F32),
            pltpu.VMEM((step, inner), F32),
            pltpu.VMEM((step, inner), F32),
            pltpu.VMEM((16, inner), F32),
        ],
        compiler_params=params("arbitrary", "arbitrary"),
        name="recur",
    )(before, rin, taps, bias.reshape(1, -1), table, gate_bias, slope.reshape(1, -1))


def shards(tokens, norm_gain, lru_proj, gelu_proj, conv_weight, conv_bias, gate_weights, gate_bias, decay_param):
    seq_count, tok_rows, width = tokens.shape
    inner = lru_proj.shape[1]
    block = gate_weights.shape[1] // 2
    heads = inner // block
    fsdp, seq = lax.axis_size("fsdp"), lax.axis_size("seq")
    me = lax.axis_index("fsdp")
    core = me % 2
    half = inner // 2

    def mine(x, which):
        split = x.reshape(x.shape[:-1] + (heads // 2, 2, block))
        return lax.dynamic_index_in_dim(split, which, split.ndim - 2, False).reshape(x.shape[:-1] + (half,))

    bits = [1 << k for k in range(1, fsdp.bit_length() - 1)]

    def gather(own, other):
        both = line_gather(jnp.concatenate([own, other]))
        high = own.shape[0]
        first = both[:, :high].reshape(-1, own.shape[1])
        second = both[:, high:].reshape(-1, own.shape[1])
        found = plane_gather(first, bits)
        found.update({k ^ 1: v for k, v in plane_gather(second, bits[::-1]).items()})
        return [found[k] for k in range(fsdp)]

    def chunked(own, other, count):
        wide = half // count
        return [gather(own[:, k * wide : (k + 1) * wide], other[:, k * wide : (k + 1) * wide]) for k in range(count)]

    lru_own, gelu_own = mine(lru_proj, core), mine(gelu_proj, core)
    lru_other = flip(mine(lru_proj, 1 - core), 1)
    gelu_other = flip(mine(gelu_proj, 1 - core), 1)
    lru_parts = chunked(lru_own, lru_other, LRU_CHUNKS)
    gelu_parts = chunked(gelu_own, gelu_other, GELU_CHUNKS)

    per_device = heads // seq
    if per_device % 2 == 0:
        piece = gate_weights.reshape(per_device // 2, 2, block, 2 * block)
        piece = lax.dynamic_index_in_dim(piece, core, 1, False)
        table = line_gather(piece).reshape(heads // 2, block, 2 * block)
    else:
        table = line_gather(gate_weights).reshape(heads // 2, 2, block, 2 * block)
        table = lax.dynamic_index_in_dim(table, core, 1, False)

    flat = tokens.reshape(seq_count * tok_rows, width)
    held, unused = lax.optimization_barrier((flat, lru_other))
    order = jnp.arange(fsdp, dtype=jnp.int32) ^ me
    normed = norm(flat, flip(held, 1), norm_gain, order)

    rin = jnp.concatenate([product(normed, parts) for parts in lru_parts], axis=1)
    seqs = 2 * seq_count
    last = rin.reshape(seqs, tok_rows, half)[:, tok_rows - 8 :]
    before = lax.ppermute(last, "seq", [(i, i + 1) for i in range(seq - 1)])
    slope = -8.0 * jax.nn.softplus(mine(decay_param, core))
    local, cumulative = recur(
        rin, before, mine(conv_weight, core), mine(conv_bias, core), table, mine(gate_bias, core), slope
    )
    ends = jnp.stack([x.reshape(seqs, tok_rows, half)[:, tok_rows - 1] for x in (cumulative, local)])
    start = jnp.zeros((seqs, half), F32)
    for hop in range(seq - 1, 0, -1):
        come = lax.ppermute(ends, "seq", [(i, i + hop) for i in range(seq - hop)])
        start = come[1] + come[0] * start
    start = start[:, None, :]

    rows = seq_count * tok_rows
    keep, got = [], []
    for k, parts in enumerate(gelu_parts):
        sent = finish(normed, parts, local, cumulative, start, k, rows, rows)
        got.append(flip(sent, 1))
        keep.append(finish(normed, parts, local, cumulative, start, k, 0, rows))
    kept = jnp.concatenate(keep, axis=1).reshape(rows, heads // 2, 1, block)
    came = jnp.concatenate(got, axis=1).reshape(rows, heads // 2, 1, block)
    out = jnp.where(core == 0, jnp.concatenate([kept, came], axis=2), jnp.concatenate([came, kept], axis=2))
    return out.reshape(seq_count, tok_rows, inner)


def solution(mesh):
    placed = (
        P("fsdp", "seq", None),
        P(),
        P(("fsdp", "seq"), None),
        P(("fsdp", "seq"), None),
        P(),
        P(),
        P("seq", None),
        P(),
        P(),
    )
    return jax.shard_map(
        shards, mesh=mesh, in_specs=placed, out_specs=P("fsdp", "seq", None), check_vma=False
    )
```

```python
import functools

import jax
import jax.numpy as jnp
from jax import lax
from jax.experimental import pallas as pl
from jax.experimental.pallas import tpu as pltpu
from jax.sharding import PartitionSpec as P

LRU_CHUNKS = 2
GELU_CHUNKS = 2
BF = jnp.bfloat16
F32 = jnp.float32


def params(*kinds):
    return pltpu.CompilerParams(dimension_semantics=kinds, vmem_limit_bytes=56 * 1024 * 1024)


def flip(x, bit):
    return lax.ppermute(x, "fsdp", [(i, i ^ bit) for i in range(lax.axis_size("fsdp"))])


def after(x, *others):
    return lax.optimization_barrier((x,) + others)[0]


def line_gather(x):
    devices = lax.axis_size("seq")
    right, left = x, x
    below, above = [], []
    for hop in range(1, devices):
        right = lax.ppermute(right, "seq", [(i, i + 1) for i in range(hop - 1, devices - 1)])
        left = lax.ppermute(left, "seq", [(i, i - 1) for i in range(1, devices - hop + 1)])
        below.append(right)
        above.append(left)
    stacked = jnp.stack(below[::-1] + [x] + above)
    begin = devices - 1 - lax.axis_index("seq")
    return lax.dynamic_slice_in_dim(stacked, begin, devices, axis=0)


def plane_gather(block, bits):
    found = {0: block}
    for bit in bits:
        found.update({offset ^ bit: flip(part, bit) for offset, part in list(found.items())})
    return found


def norm_body(order, own, other, gain, out, scratch):
    block = out.shape[2] // order.shape[0]
    for source, index in ((own, 0), (other, 1)):
        values = source[...].astype(F32)
        mean_square = jnp.mean(values * values, axis=-1, keepdims=True)
        scratch[...] = (values * lax.rsqrt(mean_square + 1e-06) * gain[...]).astype(BF)
        for position in range(order.shape[0]):
            begin = pl.multiple_of(order[position] * block, 128)
            out[index, :, position * block : (position + 1) * block] = scratch[:, pl.ds(begin, block)]


def norm(own, other, gain, order):
    rows, width = own.shape
    step = 128
    return pl.pallas_call(
        norm_body,
        grid_spec=pltpu.PrefetchScalarGridSpec(
            num_scalar_prefetch=1,
            grid=(rows // step,),
            in_specs=[
                pl.BlockSpec((step, width), lambda i, o: (i, 0)),
                pl.BlockSpec((step, width), lambda i, o: (i, 0)),
                pl.BlockSpec((1, width), lambda i, o: (0, 0)),
            ],
            out_specs=pl.BlockSpec((2, step, width), lambda i, o: (0, i, 0)),
            scratch_shapes=[pltpu.VMEM((step, width), BF)],
        ),
        out_shape=jax.ShapeDtypeStruct((2, rows, width), BF),
        compiler_params=params("arbitrary"),
        name="norm",
    )(order, own, other, gain.reshape(1, -1)).reshape(2 * rows, width)


def load_table(parts, table, sems):
    @pl.when(pl.program_id(0) == 0)
    def _():
        height = parts[0].shape[0]
        copies = [
            pltpu.make_async_copy(part, table.at[pl.ds(i * height, height)], sems.at[i])
            for i, part in enumerate(parts)
        ]
        for copy in copies:
            copy.start()
        for copy in copies:
            copy.wait()


def product_body(count, rows, *refs):
    parts, out, table, sems = refs[:count], refs[count], refs[count + 1], refs[count + 2]
    load_table(parts, table, sems)
    out[...] = jnp.dot(rows[...], table[...], preferred_element_type=F32).astype(out.dtype)


def gelu_tanh(v):
    return 0.5 * v * (1.0 + jnp.tanh(0.7978845608028654 * (v + 0.044715 * v * v * v)))


def finish_body(count, rows, local, cumulative, start, *refs):
    parts, keep, sent, table, sems = refs[:count], *refs[count:]
    load_table(parts, table, sems)
    gelu_in = jnp.dot(rows[...], table[...], preferred_element_type=F32)
    state = local[...] + cumulative[...] * start[0]
    done = (state * gelu_tanh(gelu_in)).astype(BF)
    first = pl.program_id(0) < pl.num_programs(0) // 2

    @pl.when(first)
    def _():
        keep[...] = done

    @pl.when(jnp.logical_not(first))
    def _():
        sent[...] = done


def product(rows, parts):
    total, depth = rows.shape
    width = parts[0].shape[1]
    step = 256
    count = len(parts)
    return pl.pallas_call(
        functools.partial(product_body, count),
        grid=(total // step,),
        in_specs=[pl.BlockSpec((step, depth), lambda i: (i, 0))]
        + [pl.BlockSpec(memory_space=pl.ANY)] * count,
        out_specs=pl.BlockSpec((step, width), lambda i: (i, 0)),
        out_shape=jax.ShapeDtypeStruct((total, width), BF),
        scratch_shapes=[pltpu.VMEM((depth, width), BF), pltpu.SemaphoreType.DMA((count,))],
        compiler_params=params("arbitrary"),
        name="lru_product",
    )(rows, *parts)


def finish(rows, parts, local, cumulative, start, column):
    total, depth = rows.shape
    width = parts[0].shape[1]
    step = 256
    count = len(parts)
    blocks = total // step
    per_start = total // start.shape[0] // step
    return pl.pallas_call(
        functools.partial(finish_body, count),
        grid=(blocks,),
        in_specs=[
            pl.BlockSpec((step, depth), lambda i: (i, 0)),
            pl.BlockSpec((step, width), lambda i: (i, column)),
            pl.BlockSpec((step, width), lambda i: (i, column)),
            pl.BlockSpec((1, 1, width), lambda i: (i // per_start, 0, column)),
        ]
        + [pl.BlockSpec(memory_space=pl.ANY)] * count,
        out_specs=[
            pl.BlockSpec((step, width), lambda i: (jnp.minimum(i, blocks // 2 - 1), 0)),
            pl.BlockSpec((step, width), lambda i: (jnp.maximum(i - blocks // 2, 0), 0)),
        ],
        out_shape=[jax.ShapeDtypeStruct((total // 2, width), BF)] * 2,
        scratch_shapes=[pltpu.VMEM((depth, width), BF), pltpu.SemaphoreType.DMA((count,))],
        compiler_params=params("arbitrary"),
        name="gelu_finish",
    )(rows, local, cumulative, start, *parts)


def weave_body(block, core, *refs):
    out = refs[-1]
    half = (len(refs) - 1) // 2
    at = 0
    for kept, came in zip(refs[:half], refs[half:-1]):
        for k in range(kept.shape[1] // block):
            piece = slice(k * block, (k + 1) * block)
            out[:, pl.ds(pl.multiple_of((at + core[0]) * block, block), block)] = kept[:, piece]
            out[:, pl.ds(pl.multiple_of((at + 1 - core[0]) * block, block), block)] = came[:, piece]
            at += 2


def weave(keep, got, core, block):
    rows = keep[0].shape[0]
    step = 256
    inner = 2 * sum(x.shape[1] for x in keep)
    return pl.pallas_call(
        functools.partial(weave_body, block),
        grid_spec=pltpu.PrefetchScalarGridSpec(
            num_scalar_prefetch=1,
            grid=(rows // step,),
            in_specs=[pl.BlockSpec((step, x.shape[1]), lambda i, c: (i, 0)) for x in keep + got],
            out_specs=pl.BlockSpec((step, inner), lambda i, c: (i, 0)),
        ),
        out_shape=jax.ShapeDtypeStruct((rows, inner), BF),
        compiler_params=params("arbitrary"),
        name="weave",
    )(core.astype(jnp.int32).reshape(1), *keep, *got)


def minus_expm1(y):
    series = -y * (1.0 + y * (0.5 + y * (1 / 6 + y * (1 / 24 + y * (1 / 120)))))
    return jnp.where(y > -0.1, series, 1.0 - jnp.exp(y))


def recur_body(before, rin, taps, bias, table, gate_bias, slope, local, cumulative, padded, decay, driven, carry):
    step, inner = rin.shape
    heads, block = table.shape[0], table.shape[1]

    @pl.when(pl.program_id(1) == 0)
    def _():
        padded[0:8, :] = before[0].astype(F32)
        carry[0:8, :] = jnp.zeros((8, inner), F32)
        carry[8:16, :] = jnp.ones((8, inner), F32)

    padded[8 : 8 + step, :] = rin[...].astype(F32)
    for head in range(heads):
        at = slice(head * block, (head + 1) * block)
        conv_sum = jnp.broadcast_to(bias[0:1, at], (step, block))
        for tap in range(taps.shape[0]):
            conv_sum = conv_sum + taps[tap : tap + 1, at] * padded[8 - tap : 8 - tap + step, at]
        conv_out = conv_sum.astype(BF)
        gates = jnp.dot(conv_out, table[head], preferred_element_type=F32)
        input_gate = jax.nn.sigmoid(gates[:, :block] + gate_bias[0:1, at])
        recur_gate = jax.nn.sigmoid(gates[:, block:] + gate_bias[1:2, at])
        log_decay = slope[0:1, at] * recur_gate
        decay[:, at] = jnp.exp(log_decay)
        driven[:, at] = jnp.sqrt(minus_expm1(2.0 * log_decay)) * input_gate * conv_out.astype(F32)
    padded[0:8, :] = padded[step : step + 8, :]
    row = lax.broadcasted_iota(jnp.int32, (8, inner), 0)

    def advance(group, carried):
        state, prefix = carried
        at = pl.ds(pl.multiple_of(group * 8, 8), 8)
        a, b = decay[at, :], driven[at, :]
        for shift in (1, 2, 4):
            keep = row >= shift
            b = b + a * jnp.where(keep, pltpu.roll(b, shift, 0), 0.0)
            a = a * jnp.where(keep, pltpu.roll(a, shift, 0), 1.0)
        state = b + a * state
        prefix = a * prefix
        local[at, :] = state
        cumulative[at, :] = prefix
        return (
            jnp.broadcast_to(state[7:8, :], (8, inner)),
            jnp.broadcast_to(prefix[7:8, :], (8, inner)),
        )

    state, prefix = lax.fori_loop(0, step // 8, advance, (carry[0:8, :], carry[8:16, :]))
    carry[0:8, :] = state
    carry[8:16, :] = prefix


def recur(rin, before, taps, bias, table, gate_bias, slope):
    total, inner = rin.shape
    seqs = before.shape[0]
    step = 128
    blocks = total // seqs // step
    whole = lambda shape: pl.BlockSpec(shape, lambda s, t: (0,) * len(shape))
    rows = pl.BlockSpec((step, inner), lambda s, t: (s * blocks + t, 0))
    return pl.pallas_call(
        recur_body,
        grid=(seqs, blocks),
        in_specs=[
            pl.BlockSpec((1, 8, inner), lambda s, t: (s, 0, 0)),
            rows,
            whole(taps.shape),
            whole((1, inner)),
            whole(table.shape),
            whole((2, inner)),
            whole((1, inner)),
        ],
        out_specs=[rows, rows],
        out_shape=[jax.ShapeDtypeStruct((total, inner), F32)] * 2,
        scratch_shapes=[
            pltpu.VMEM((step + 8, inner), F32),
            pltpu.VMEM((step, inner), F32),
            pltpu.VMEM((step, inner), F32),
            pltpu.VMEM((16, inner), F32),
        ],
        compiler_params=params("arbitrary", "arbitrary"),
        name="recur",
    )(before, rin, taps, bias.reshape(1, -1), table, gate_bias, slope.reshape(1, -1))


def shards(tokens, norm_gain, lru_proj, gelu_proj, conv_weight, conv_bias, gate_weights, gate_bias, decay_param):
    seq_count, tok_rows, width = tokens.shape
    inner = lru_proj.shape[1]
    block = gate_weights.shape[1] // 2
    heads = inner // block
    fsdp, seq = lax.axis_size("fsdp"), lax.axis_size("seq")
    me = lax.axis_index("fsdp")
    core = me % 2
    half = inner // 2

    def mine(x, which):
        split = x.reshape(x.shape[:-1] + (heads // 2, 2, block))
        return lax.dynamic_index_in_dim(split, which, split.ndim - 2, False).reshape(x.shape[:-1] + (half,))

    bits = [1 << k for k in range(1, fsdp.bit_length() - 1)]

    def spread(both, high):
        wide = both.shape[-1]
        first, second = both[:, :high].reshape(-1, wide), both[:, high:].reshape(-1, wide)
        found = plane_gather(first, bits)
        found.update({k ^ 1: v for k, v in plane_gather(second, bits[::-1]).items()})
        return [found[k] for k in range(fsdp)]

    def pieces(own, other, count):
        wide = half // count
        return [
            jnp.concatenate([own[:, k * wide : (k + 1) * wide], other[:, k * wide : (k + 1) * wide]])
            for k in range(count)
        ]

    high = lru_proj.shape[0]
    flat = tokens.reshape(seq_count * tok_rows, width)
    lru_own, gelu_own = mine(lru_proj, core), mine(gelu_proj, core)
    lru_other = flip(mine(lru_proj, 1 - core), 1)
    gelu_other = flip(after(mine(gelu_proj, 1 - core), lru_other), 1)
    other_flat = flip(after(flat, gelu_other), 1)
    waiting = pieces(lru_own, lru_other, LRU_CHUNKS) + pieces(gelu_own, gelu_other, GELU_CHUNKS)
    order = jnp.arange(fsdp, dtype=jnp.int32) ^ me

    both = line_gather(waiting[0])
    lru_parts = [spread(both, high)]
    normed = norm(after(flat, both), other_flat, norm_gain, order)
    both = line_gather(after(waiting[1], both))
    lru_parts.append(spread(both, high))
    both = line_gather(after(waiting[2], both, normed))
    gelu_parts = [spread(both, high)]

    per_device = heads // seq
    if per_device % 2 == 0:
        piece = gate_weights.reshape(per_device // 2, 2, block, 2 * block)
        piece = lax.dynamic_index_in_dim(piece, core, 1, False)
        table = line_gather(after(piece, both)).reshape(heads // 2, block, 2 * block)
    else:
        table = line_gather(after(gate_weights, both)).reshape(heads // 2, 2, block, 2 * block)
        table = lax.dynamic_index_in_dim(table, core, 1, False)

    first_rin = product(normed, lru_parts[0])
    both = line_gather(after(waiting[3], table, first_rin))
    gelu_parts.append(spread(both, high))
    rin = jnp.concatenate([first_rin, product(normed, lru_parts[1])], axis=1)
    seqs = 2 * seq_count
    last = rin.reshape(seqs, tok_rows, half)[:, tok_rows - 8 :]
    before = lax.ppermute(last, "seq", [(i, i + 1) for i in range(seq - 1)])
    slope = -8.0 * jax.nn.softplus(mine(decay_param, core))
    local, cumulative = recur(
        rin, before, mine(conv_weight, core), mine(conv_bias, core), table, mine(gate_bias, core), slope
    )
    ends = jnp.stack([x.reshape(seqs, tok_rows, half)[:, tok_rows - 1] for x in (cumulative, local)])
    start = jnp.zeros((seqs, half), F32)
    for hop in range(seq - 1, 0, -1):
        come = lax.ppermute(ends, "seq", [(i, i + hop) for i in range(seq - hop)])
        start = come[1] + come[0] * start
    start = start[:, None, :]

    keep, got = [], []
    for k, parts in enumerate(gelu_parts):
        kept, sent = finish(normed, parts, local, cumulative, start, k)
        keep.append(kept)
        got.append(flip(sent, 1))
    return weave(keep, got, core, block).reshape(seq_count, tok_rows, inner)


def solution(mesh):
    placed = (
        P("fsdp", "seq", None),
        P(),
        P(("fsdp", "seq"), None),
        P(("fsdp", "seq"), None),
        P(),
        P(),
        P("seq", None),
        P(),
        P(),
    )
    return jax.shard_map(
        shards, mesh=mesh, in_specs=placed, out_specs=P("fsdp", "seq", None), check_vma=False
    )
```
